8 devices in a mesh: part: 1 (over z), col: 2 (over y), row: 4 (over x, core).
Axes of the slice: x: 2, y: 2, z: 1, core: 2. Of those that a mesh axis runs over, the one named last changes fastest.
Arguments:
- l_in: float32 [192, 64, 12288], P(('part', 'row'), None, 'col')
Outputs:
- output 1: float32 [192, 64, 12288], P(('part', 'row'), None, 'col')
- output 2: float32 [4, 128, 64], P('part')
- output 3: float32 [4, 12288, 64], P(None, ('part', 'row'))
- output 4: float32 [4, 64, 64], P('part')
All inputs are finite; a program needn't handle non-finite values.
Results may differ from the reference program's by a relative error of at most 0.001.
Values sent between devices are 32-bit elements.
A program may use at most 1 GiB of HBM per device.

```python
import jax
import jax.numpy as jnp
from jax import lax

MAT_ORDER = 12288
BLOCK_SIZE = 64
NUM_PANELS = 4
PROC_ROWS = 4
PROC_COLS = 2

PREC_HIGH = lax.Precision.HIGHEST


def mat_dot(left, right):
    return jnp.dot(left, right, precision=PREC_HIGH, preferred_element_type=jnp.float32)


def to_natural(stored):
    blocks = stored.reshape(PROC_ROWS, MAT_ORDER // (PROC_ROWS * BLOCK_SIZE), BLOCK_SIZE, PROC_COLS, MAT_ORDER // (PROC_COLS * BLOCK_SIZE), BLOCK_SIZE)
    return blocks.transpose(1, 0, 2, 4, 3, 5).reshape(MAT_ORDER, MAT_ORDER)


def to_stored(natural):
    blocks = natural.reshape(MAT_ORDER // (PROC_ROWS * BLOCK_SIZE), PROC_ROWS, BLOCK_SIZE, MAT_ORDER // (PROC_COLS * BLOCK_SIZE), PROC_COLS, BLOCK_SIZE)
    return blocks.transpose(1, 0, 2, 4, 3, 5).reshape(MAT_ORDER, MAT_ORDER)


def rows_to_stored(natural):
    blocks = natural.reshape(NUM_PANELS, MAT_ORDER // (PROC_ROWS * BLOCK_SIZE), PROC_ROWS, BLOCK_SIZE, BLOCK_SIZE)
    return blocks.transpose(0, 2, 1, 3, 4).reshape(NUM_PANELS, MAT_ORDER, BLOCK_SIZE)


def setup_inputs(seed: int = 0, part: int = 0) -> dict:
    draw_key = jax.random.fold_in(jax.random.key(seed), part)
    gauss_mat = jax.random.normal(draw_key, (MAT_ORDER, MAT_ORDER), jnp.float32)
    sym_mat = (gauss_mat + gauss_mat.T) * (0.5 ** 0.5)
    stored = to_stored(jnp.tril(sym_mat))
    return {"l_in": stored.reshape(MAT_ORDER // BLOCK_SIZE, BLOCK_SIZE, MAT_ORDER)}


def householder_panel(panel):
    row_ids = jnp.arange(panel.shape[0])
    col_ids = jnp.arange(BLOCK_SIZE)

    def qr_column(col_idx, carry):
        work, vecs, tau_vec = carry
        column = lax.dynamic_index_in_dim(work, col_idx, axis=1, keepdims=False)
        below = jnp.where(row_ids >= col_idx, column, 0.0)
        alpha_val = lax.dynamic_index_in_dim(column, col_idx, keepdims=False)
        norm_x = jnp.sqrt(jnp.sum(below * below))
        beta_val = jnp.where(alpha_val >= 0.0, -norm_x, norm_x)
        tau_val = (beta_val - alpha_val) / beta_val
        house = jnp.where(row_ids == col_idx, 1.0, jnp.where(row_ids > col_idx, below / (alpha_val - beta_val), 0.0))
        proj = jnp.dot(house, work, precision=PREC_HIGH, preferred_element_type=jnp.float32)
        proj = jnp.where(col_ids > col_idx, proj, 0.0)
        work = work - tau_val * house[:, None] * proj[None, :]
        new_col = jnp.where(row_ids < col_idx, column, jnp.where(row_ids == col_idx, beta_val, 0.0))
        pick = (col_ids == col_idx)[None, :]
        work = jnp.where(pick, new_col[:, None], work)
        vecs = jnp.where(pick, house[:, None], vecs)
        tau_vec = jnp.where(col_ids == col_idx, tau_val, tau_vec)
        return work, vecs, tau_vec

    begin = (panel, jnp.zeros_like(panel), jnp.zeros((BLOCK_SIZE,), jnp.float32))
    work, vecs, tau_vec = lax.fori_loop(0, BLOCK_SIZE, qr_column, begin)
    return vecs, tau_vec, work[:BLOCK_SIZE]


def triangular_factor(tau_vec, gram):
    col_ids = jnp.arange(BLOCK_SIZE)

    def t_column(col_idx, tri_mat):
        g_col = jnp.where(col_ids < col_idx, lax.dynamic_index_in_dim(gram, col_idx, axis=1, keepdims=False), 0.0)
        tau_val = lax.dynamic_index_in_dim(tau_vec, col_idx, keepdims=False)
        new_col = jnp.where(col_ids == col_idx, tau_val, -tau_val * jnp.dot(tri_mat, g_col, precision=PREC_HIGH, preferred_element_type=jnp.float32))
        return jnp.where((col_ids == col_idx)[None, :], new_col[:, None], tri_mat)

    return lax.fori_loop(0, BLOCK_SIZE, t_column, jnp.zeros((BLOCK_SIZE, BLOCK_SIZE), jnp.float32))


def reference(l_in):
    lower = to_natural(l_in.reshape(MAT_ORDER, MAT_ORDER))
    work = lower + jnp.tril(lower, -1).T
    band_list = []
    vec_list = []
    tri_list = []
    for panel_idx in range(NUM_PANELS):
        diag_blk = jnp.tril(work[:BLOCK_SIZE, :BLOCK_SIZE])
        vecs, tau_vec, r_blk = householder_panel(work[BLOCK_SIZE:, :BLOCK_SIZE])
        t_mat = triangular_factor(tau_vec, mat_dot(vecs.T, vecs))
        trail = work[BLOCK_SIZE:, BLOCK_SIZE:]
        y_mat = mat_dot(mat_dot(trail, vecs), t_mat)
        m_mat = mat_dot(t_mat.T, mat_dot(vecs.T, y_mat))
        w_mat = y_mat - 0.5 * mat_dot(vecs, m_mat)
        work = trail - mat_dot(vecs, w_mat.T) - mat_dot(w_mat, vecs.T)
        band_list.append(jnp.concatenate([diag_blk, r_blk], axis=0))
        vec_list.append(jnp.pad(vecs, (((panel_idx + 1) * BLOCK_SIZE, 0), (0, 0))))
        tri_list.append(t_mat)
    done_rows = NUM_PANELS * BLOCK_SIZE
    l_nat = jnp.pad(jnp.tril(work), ((done_rows, 0), (done_rows, 0)))
    l_out = to_stored(l_nat).reshape(MAT_ORDER // BLOCK_SIZE, BLOCK_SIZE, MAT_ORDER)
    return l_out, jnp.stack(band_list), rows_to_stored(jnp.stack(vec_list)), jnp.stack(tri_list)
```

```python
import functools

import jax
import jax.numpy as jnp
from jax import lax
from jax.experimental import pallas as pl
from jax.experimental.pallas import tpu as pltpu
from jax.sharding import PartitionSpec as P

PANELS = 4
NB = 64
NB3 = 3 * NB
LANES = 128
N = 12288
HALF = N // 2
ROWS = N // 4
F32 = jnp.float32
BF16 = jnp.bfloat16
CH = 2048
NCH = N // CH
TR, TC = 512, 1024
NT = ROWS // TR
VMEM_LIMIT = 62 * 1024 * 1024


def lane_of_block(blk):
    pos = (blk % 2) * HALF + (blk // 2) * NB
    return pos // LANES, pos % LANES


def span(start, size):
    return pl.ds(pl.multiple_of(start, size), size)


def split3(x):
    x1 = x.astype(BF16)
    r = x - x1.astype(F32)
    x2 = r.astype(BF16)
    x3 = (r - x2.astype(F32)).astype(BF16)
    return x1, x2, x3


def dot_nn(a, b):
    return lax.dot_general(a, b, (((1,), (0,)), ((), ())), preferred_element_type=F32)


def dot_nt(a, b):
    return lax.dot_general(a, b, (((1,), (1,)), ((), ())), preferred_element_type=F32)


def hi_nn(a, b):
    return lax.dot_general(a, b, (((1,), (0,)), ((), ())), precision=lax.Precision.HIGHEST, preferred_element_type=F32)


def hi_tn(a, b):
    return lax.dot_general(a, b, (((0,), (0,)), ((), ())), precision=lax.Precision.HIGHEST, preferred_element_type=F32)


def stack3(x):
    return jnp.concatenate(split3(x), axis=0)


def fold9(acc):
    r = acc[0:NB] + (acc[NB:LANES] + acc[LANES:NB3])
    return r[:, 0:NB] + (r[:, NB:LANES] + r[:, LANES:NB3])


def small_by_wide(c_stack, b):
    b1, b2, b3 = split3(b)
    r1 = dot_nn(c_stack, b1)
    r2 = dot_nn(c_stack[0:LANES], b2)
    r3 = dot_nn(c_stack[0:NB], b3)
    return r1[0:NB] + ((r1[NB:LANES] + r2[0:NB]) + (r1[LANES:NB3] + (r2[NB:LANES] + r3)))


def iota2(shape, dim):
    return lax.broadcasted_iota(jnp.int32, shape, dim)


def params(**kw):
    return pltpu.CompilerParams(vmem_limit_bytes=VMEM_LIMIT, **kw)


def interleave_kernel(a_ref, b_ref, o_ref):
    lo = iota2((NB, LANES), 1) < NB
    for m in range(12):
        a = a_ref[0, :, m * LANES:(m + 1) * LANES]
        b = b_ref[0, :, m * LANES:(m + 1) * LANES]
        o_ref[0, :, (2 * m) * LANES:(2 * m + 1) * LANES] = jnp.where(lo, a, pltpu.roll(b, NB, 1))
        o_ref[0, :, (2 * m + 1) * LANES:(2 * m + 2) * LANES] = jnp.where(lo, pltpu.roll(a, NB, 1), b)


def interleave(gathered):
    width = 12 * LANES
    return pl.pallas_call(
        interleave_kernel,
        grid=(2, 2, 2),
        in_specs=[
            pl.BlockSpec((1, NB, width), lambda q, c, m: (q * 4 + c, 0, m)),
            pl.BlockSpec((1, NB, width), lambda q, c, m: (q * 4 + c + 2, 0, m)),
        ],
        out_specs=pl.BlockSpec((1, NB, 2 * width), lambda q, c, m: (q, 0, c * 2 + m)),
        out_shape=jax.ShapeDtypeStruct((2, NB, N), F32),
        compiler_params=params(),
        name="interleave",
    )(gathered, gathered)


def qr_kernel(k, p_ref, vt_ref, vts_ref, band_ref, t_ref, xb_ref, rt_ref, inv_ref, tau_ref, gram_ref):
    piv_tile, piv_off = lane_of_block(k + 1)
    diag_tile, diag_off = lane_of_block(k)
    piv = slice(piv_tile * LANES, piv_tile * LANES + LANES)

    def copy_in(c, _):
        at = span(c * CH, CH)
        vt_ref[:, at] = p_ref[:, at]
        return 0

    lax.fori_loop(0, NCH, copy_in, 0)
    lane64 = iota2((NB, LANES), 1)
    row64 = iota2((NB, LANES), 0)
    for cls in range(2):
        sl = slice(cls * HALF, cls * HALF + LANES)
        blk = 2 * (lane64 // NB) + cls
        vt_ref[:, sl] = jnp.where(blk >= k + 1, p_ref[:, sl], 0.0)
    rt_ref[...] = jnp.zeros_like(rt_ref)
    inv_ref[...] = jnp.zeros_like(inv_ref)
    tau_ref[...] = jnp.zeros_like(tau_ref)

    for g0 in range(8):
        r0 = 8 * g0
        groups = 8 - g0
        height = 8 * groups
        lane = iota2((height, LANES), 1)
        row_b = r0 + iota2((height, LANES), 0)
        row1 = r0 + iota2((height, 1), 0)

        def step(jj, _, r0=r0, groups=groups, height=height, lane=lane, row_b=row_b, row1=row1):
            j = r0 + jj
            at_piv = lane == piv_off + j

            def dots(c, accs):
                at = span(c * CH, CH)
                xb = jnp.broadcast_to(vt_ref[pl.ds(j, 1), at], (8, CH))
                xb_ref[:, at] = xb
                out = []
                for g in range(groups):
                    prod = vt_ref[r0 + 8 * g:r0 + 8 * g + 8, at] * xb
                    parts = [prod[:, t * LANES:(t + 1) * LANES] for t in range(CH // LANES)]
                    while len(parts) > 1:
                        parts = [parts[i] + parts[i + 1] for i in range(0, len(parts), 2)]
                    out.append(accs[g] + parts[0])
                return tuple(out)

            accs = lax.fori_loop(0, NCH, dots, tuple(jnp.zeros((8, LANES), F32) for _ in range(groups)))
            d = jnp.sum(jnp.concatenate(accs, axis=0), axis=1, keepdims=True)
            pv = jnp.sum(jnp.where(at_piv, vt_ref[r0:NB, piv], 0.0), axis=1, keepdims=True)
            is_j = row1 == j
            nrm2 = jnp.sum(jnp.where(is_j, d, 0.0), axis=0, keepdims=True)
            alpha = jnp.sum(jnp.where(is_j, pv, 0.0), axis=0, keepdims=True)
            norm = jnp.sqrt(nrm2)
            beta = jnp.where(alpha >= 0.0, -norm, norm)
            tau = (beta - alpha) / beta
            inv = 1.0 / (alpha - beta)
            proj = inv * (d - beta * pv)
            s = jnp.where(row1 > j, tau * proj * inv, 0.0)
            xb_ref[:, piv] = xb_ref[:, piv] - jnp.where(lane[0:8] == piv_off + j, beta, 0.0)
            sb = jnp.broadcast_to(s, (height, LANES))

            def update(c, _):
                at = span(c * CH, CH)
                xb = xb_ref[:, at]
                for g in range(groups):
                    sg = sb[8 * g:8 * g + 8]
                    blk = vt_ref[r0 + 8 * g:r0 + 8 * g + 8, at]
                    vt_ref[r0 + 8 * g:r0 + 8 * g + 8, at] = jnp.concatenate(
                        [blk[:, t * LANES:(t + 1) * LANES] - sg * xb[:, t * LANES:(t + 1) * LANES] for t in range(CH // LANES)], axis=1)
                return 0

            lax.fori_loop(0, NCH, update, 0)
            r_col = jnp.where(is_j, beta, jnp.where(row1 > j, pv - s * (alpha - beta), 0.0))
            rt_ref[r0:NB] = jnp.where(lane == j, r_col, rt_ref[r0:NB])
            vt_ref[r0:NB, piv] = jnp.where(at_piv & (row_b > j), 0.0, vt_ref[r0:NB, piv])
            inv_ref[r0:NB] = jnp.where(row_b == j, inv, inv_ref[r0:NB])
            tau_ref[r0:NB] = jnp.where(row_b == j, tau, tau_ref[r0:NB])
            return 0

        lax.fori_loop(0, 8, step, 0)

    vt_ref[:, piv] = jnp.where(lane64 == piv_off + row64, 0.0, vt_ref[:, piv])
    inv_b = inv_ref[...]
    gram_ref[...] = jnp.zeros_like(gram_ref)

    def finish(c, _):
        at = span(c * CH, CH)
        blk = vt_ref[:, at]
        blk = jnp.concatenate([blk[:, t * LANES:(t + 1) * LANES] * inv_b for t in range(CH // LANES)], axis=1)
        lanes = c * CH + iota2((NB, CH), 1)
        blk = jnp.where(lanes == piv_tile * LANES + piv_off + iota2((NB, CH), 0), 1.0, blk)
        vt_ref[:, at] = blk
        st = stack3(blk)
        vts_ref[:, at] = st
        gram_ref[...] += dot_nt(st, st)
        return 0

    lax.fori_loop(0, NCH, finish, 0)
    gram = fold9(gram_ref[...])
    rr = iota2((NB, NB), 0)
    cc = iota2((NB, NB), 1)
    t_mat = jnp.where(rr == cc, tau_ref[:, 0:NB], 0.0)
    size = 1
    while size < NB:
        pair = (rr // (2 * size) == cc // (2 * size)) & ((rr // size) % 2 == 0) & ((cc // size) % 2 == 1)
        t_mat = t_mat - hi_nn(t_mat, hi_nn(jnp.where(pair, gram, 0.0), t_mat))
        size *= 2
    t_ref[...] = t_mat
    diag = p_ref[:, diag_tile * LANES:diag_tile * LANES + LANES].T[diag_off:diag_off + NB]
    band_ref[0:NB] = jnp.where(rr >= cc, diag, 0.0)
    band_ref[NB:LANES] = rt_ref[...].T[0:NB]


def panel_qr(k, panel):
    return pl.pallas_call(
        functools.partial(qr_kernel, k),
        out_shape=(
            jax.ShapeDtypeStruct((NB, N), F32),
            jax.ShapeDtypeStruct((NB3, N), BF16),
            jax.ShapeDtypeStruct((LANES, NB), F32),
            jax.ShapeDtypeStruct((NB, NB), F32),
        ),
        scratch_shapes=[
            pltpu.VMEM((8, N), F32),
            pltpu.VMEM((NB, LANES), F32),
            pltpu.VMEM((NB, LANES), F32),
            pltpu.VMEM((NB, LANES), F32),
            pltpu.VMEM((NB3, NB3), F32),
        ],
        compiler_params=params(),
        name=f"panel_qr{k}",
    )(panel)


LOWER_TILES = [(i, j) for i in range(NT) for j in range(i + 1)]


def global_ids(pq_ref, tile_i, tile_j, shape):
    rloc = tile_i * TR + iota2(shape, 0)
    cloc = tile_j * TC + iota2(shape, 1)
    row = ((rloc >> 6) * 4 + pq_ref[0]) * NB + (rloc & 63)
    col = ((cloc >> 6) * 2 + pq_ref[1]) * NB + (cloc & 63)
    return row, col


def av_kernel(ti_ref, tj_ref, pq_ref, l_ref, vtc_ref, vtp_ref, z_ref, vrt_ref, vr_ref, ls_ref, vtr_ref, acc1_ref, acc2_ref):
    step = pl.program_id(0)
    ti = ti_ref[step]
    tj = tj_ref[step]
    proc_row = pq_ref[0]
    proc_col = pq_ref[1]
    upper = (proc_row >> 1) == 1

    @pl.when(step == 0)
    def _():
        acc1_ref[...] = jnp.zeros_like(acc1_ref)
        acc2_ref[...] = jnp.zeros_like(acc2_ref)

        def pick(i, _):
            tile = vtp_ref[:, span(i * LANES, LANES)].T
            vr_ref[span(i * NB, NB), :] = jnp.where(upper, tile[NB:LANES], tile[0:NB])
            return 0

        lax.fori_loop(0, 48, pick, 0)

        def back(m, _):
            tile = vr_ref[span(m * LANES, LANES), :].T
            vrt_ref[:, span(m * LANES, LANES)] = tile
            vtr_ref[:, span(m * LANES, LANES)] = stack3(tile)
            return 0

        lax.fori_loop(0, 24, back, 0)

    def put(tile):
        s1, s2, s3 = split3(tile)
        ls_ref[0] = s1
        ls_ref[1] = s2
        ls_ref[2] = s3

    @pl.when(ti == tj)
    def _():
        row, col = global_ids(pq_ref, ti, tj, (TR, TC))
        put(jnp.where(row == col, 0.5, 1.0) * l_ref[...])

    @pl.when(ti != tj)
    def _():
        put(l_ref[...])

    cols = span(tj * TC, TC)
    rows = span(ti * TR, TR)
    vc = vtc_ref[:, cols]
    acc1_ref[rows, :] += dot_nt(ls_ref[0], vc) + (dot_nt(ls_ref[1], vc) + dot_nt(ls_ref[2], vc))
    vr = vtr_ref[:, rows]
    acc2_ref[:, cols] += dot_nn(vr, ls_ref[0]) + (dot_nn(vr, ls_ref[1]) + dot_nn(vr, ls_ref[2]))

    @pl.when(step == len(LOWER_TILES) - 1)
    def _():
        def out(i, _):
            at = span(i * LANES, LANES)
            blk = acc1_ref[span(i * NB, NB), :]
            blk = blk[:, 0:NB] + (blk[:, NB:LANES] + blk[:, LANES:NB3])
            wide = jnp.concatenate([jnp.where(upper, 0.0, blk), jnp.where(upper, blk, 0.0)], axis=0).T
            own = acc2_ref[0:NB, at] + (acc2_ref[NB:LANES, at] + acc2_ref[LANES:NB3, at])
            for cls in range(2):
                z_ref[:, span(cls * HALF + i * LANES, LANES)] = (
                    jnp.where(proc_col == cls, own, 0.0) + jnp.where((proc_row & 1) == cls, wide, 0.0))
            return 0

        lax.fori_loop(0, 48, out, 0)


def times_matrix(pq, l_loc, vt, vts):
    tile_i = jnp.array([t[0] for t in LOWER_TILES], jnp.int32)
    tile_j = jnp.array([t[1] for t in LOWER_TILES], jnp.int32)
    return pl.pallas_call(
        av_kernel,
        grid_spec=pltpu.PrefetchScalarGridSpec(
            num_scalar_prefetch=3,
            grid=(len(LOWER_TILES),),
            in_specs=[
                pl.BlockSpec((TR, TC), lambda s, ti, tj, pq: (ti[s], tj[s])),
                pl.BlockSpec((NB3, HALF), lambda s, ti, tj, pq: (0, pq[1])),
                pl.BlockSpec((NB, HALF), lambda s, ti, tj, pq: (0, pq[0] & 1)),
            ],
            out_specs=[
                pl.BlockSpec((NB, N), lambda s, ti, tj, pq: (0, 0)),
                pl.BlockSpec((NB, ROWS), lambda s, ti, tj, pq: (0, 0)),
            ],
            scratch_shapes=[
                pltpu.VMEM((ROWS, NB), F32),
                pltpu.VMEM((3, TR, TC), BF16),
                pltpu.VMEM((NB3, ROWS), BF16),
                pltpu.VMEM((ROWS, NB3), F32),
                pltpu.VMEM((NB3, HALF), F32),
            ],
        ),
        out_shape=(jax.ShapeDtypeStruct((NB, N), F32), jax.ShapeDtypeStruct((NB, ROWS), F32)),
        compiler_params=params(),
        name="times_matrix",
    )(tile_i, tile_j, pq, l_loc, vts, vt)


WCH = 1024


def w_kernel(k, *refs):
    z_ref, vt_ref, vts_ref, t_ref = refs[:4]
    prev = refs[4:4 + 2 * k]
    rest = refs[4 + 2 * k:]
    last = k == PANELS - 1
    if last:
        w_ref, sacc_ref = rest[:2]
        cacc = rest[2:]
    else:
        a0_ref, w_ref, p_ref, sacc_ref = rest[:4]
        cacc = rest[4:]
    sacc_ref[...] = jnp.zeros_like(sacc_ref)
    for ref in cacc:
        ref[...] = jnp.zeros_like(ref)

    def sums(c, _):
        at = span(c * WCH, WCH)
        vs = vts_ref[:, at]
        sacc_ref[...] += dot_nt(vs, stack3(z_ref[:, at]))
        for ref, src in zip(cacc, prev):
            ref[...] += dot_nt(stack3(src[:, at]), vs)
        return 0

    lax.fori_loop(0, N // WCH, sums, 0)
    t_mat = t_ref[...]
    s_mat = fold9(sacc_ref[...])
    coef = [fold9(ref[...]) for ref in cacc]
    for j in range(k):
        c_v, c_w = coef[2 * j], coef[2 * j + 1]
        s_mat = s_mat - (hi_tn(c_v, c_w) + hi_tn(c_w, c_v))
    m_mat = hi_tn(t_mat, hi_nn(s_mat, t_mat))
    terms = [stack3(t_mat.T), stack3((-0.5 * m_mat).T)]
    for j in range(k):
        terms.append(stack3((-hi_nn(coef[2 * j + 1], t_mat)).T))
        terms.append(stack3((-hi_nn(coef[2 * j], t_mat)).T))
    srcs = [z_ref, vt_ref] + list(prev)

    def write_w(c, _):
        at = span(c * WCH, WCH)
        acc = small_by_wide(terms[0], srcs[0][:, at])
        for term, src in zip(terms[1:], srcs[1:]):
            acc = acc + small_by_wide(term, src[:, at])
        w_ref[:, at] = acc
        return 0

    lax.fori_loop(0, N // WCH, write_w, 0)
    lane64 = iota2((NB, LANES), 1)
    for cls in range(2):
        sl = slice(cls * HALF, cls * HALF + LANES)
        w_ref[:, sl] = jnp.where(2 * (lane64 // NB) + cls >= k + 1, w_ref[:, sl], 0.0)
    if last:
        return
    tile, off = lane_of_block(k + 1)
    pairs = [(prev[2 * j], prev[2 * j + 1]) for j in range(k)] + [(vt_ref, w_ref)]
    facs = []
    for v, w in pairs:
        v_rows = v[:, tile * LANES:tile * LANES + LANES].T[off:off + NB]
        w_rows = w[:, tile * LANES:tile * LANES + LANES].T[off:off + NB]
        facs.append((stack3(w_rows), v))
        facs.append((stack3(v_rows), w))

    def write_p(c, _):
        at = span(c * WCH, WCH)
        acc = small_by_wide(facs[0][0], facs[0][1][:, at])
        for fac, src in facs[1:]:
            acc = acc + small_by_wide(fac, src[:, at])
        p_ref[:, at] = a0_ref[:, at] - acc
        return 0

    lax.fori_loop(0, N // WCH, write_p, 0)


def make_w(k, z, vt, vts, t_mat, prev, a0_next):
    last = k == PANELS - 1
    outs = [jax.ShapeDtypeStruct((NB, N), F32)] * (1 if last else 2)
    args = [z, vt, vts, t_mat, *prev] + ([] if last else [a0_next])
    res = pl.pallas_call(
        functools.partial(w_kernel, k),
        out_shape=tuple(outs),
        scratch_shapes=[pltpu.VMEM((NB3, NB3), F32)] * (1 + 2 * k),
        compiler_params=params(),
        name=f"make_w{k}",
    )(*args)
    return (res[0], None) if last else res


PCH = 512


def prep_kernel(pq_ref, *refs):
    vr, wr, vc, wc = refs[0:4], refs[4:8], refs[8:12], refs[12:16]
    x_ref, y_ref = refs[16:]
    upper = (pq_ref[0] >> 1) == 1
    for pos, group in enumerate((vr, wr)):
        for pair in range(2):
            two = jnp.concatenate([group[2 * pair][...], group[2 * pair + 1][...]], axis=0).T
            half = jnp.concatenate(
                [jnp.where(upper, two[LANES * i + NB:LANES * i + LANES], two[LANES * i:LANES * i + NB]) for i in range(PCH // LANES)], axis=0)
            lanes = slice((2 * pos + pair) * LANES, (2 * pos + pair) * LANES + LANES)
            for s, part in enumerate(split3(half)):
                x_ref[s, :, lanes] = part
    for pos, group in enumerate((wc, vc)):
        for j in range(4):
            rows = slice((4 * pos + j) * NB, (4 * pos + j) * NB + NB)
            for s, part in enumerate(split3(group[j][...])):
                y_ref[s, rows, :] = part


def prep(pq, vts, wts):
    row_spec = pl.BlockSpec((NB, PCH), lambda c, pq: (0, (pq[0] & 1) * (HALF // PCH) + c))
    col_spec = pl.BlockSpec((NB, PCH), lambda c, pq: (0, pq[1] * (HALF // PCH) + c))
    return pl.pallas_call(
        prep_kernel,
        grid_spec=pltpu.PrefetchScalarGridSpec(
            num_scalar_prefetch=1,
            grid=(HALF // PCH,),
            in_specs=[row_spec] * 8 + [col_spec] * 8,
            out_specs=[
                pl.BlockSpec((3, PCH // 2, 512), lambda c, pq: (0, c, 0)),
                pl.BlockSpec((3, 512, PCH), lambda c, pq: (0, 0, c)),
            ],
        ),
        out_shape=(jax.ShapeDtypeStruct((3, ROWS, 512), BF16), jax.ShapeDtypeStruct((3, 512, HALF), BF16)),
        compiler_params=params(),
        name="prep",
    )(pq, *vts, *wts, *vts, *wts)


def final_kernel(pq_ref, l_ref, x_ref, y_ref, o_ref):
    ti = pl.program_id(0)
    tj = pl.program_id(1)

    @pl.when(tj > ti)
    def _():
        o_ref[...] = jnp.zeros_like(o_ref)

    @pl.when(tj <= ti)
    def _():
        x1, x2, x3 = x_ref[0], x_ref[1], x_ref[2]
        width = 256
        for c in range(TC // width):
            cols = slice(c * width, (c + 1) * width)
            y1, y2, y3 = y_ref[0, :, cols], y_ref[1, :, cols], y_ref[2, :, cols]
            upd = dot_nn(x3, y1) + dot_nn(x1, y3) + dot_nn(x2, y2) + dot_nn(x2, y1) + dot_nn(x1, y2) + dot_nn(x1, y1)
            rloc = ti * TR + iota2((TR, width), 0)
            cloc = tj * TC + c * width + iota2((TR, width), 1)
            row = ((rloc >> 6) * 4 + pq_ref[0]) * NB + (rloc & 63)
            col = ((cloc >> 6) * 2 + pq_ref[1]) * NB + (cloc & 63)
            keep = (row >= col) & (col >= PANELS * NB)
            o_ref[:, cols] = jnp.where(keep, l_ref[:, cols] - upd, 0.0)


def final_update(pq, l_loc, x, y):
    return pl.pallas_call(
        final_kernel,
        grid_spec=pltpu.PrefetchScalarGridSpec(
            num_scalar_prefetch=1,
            grid=(NT, NT),
            in_specs=[
                pl.BlockSpec((TR, TC), lambda i, j, pq: (i, jnp.minimum(i, j))),
                pl.BlockSpec((3, TR, 512), lambda i, j, pq: (0, i, 0)),
                pl.BlockSpec((3, 512, TC), lambda i, j, pq: (0, 0, jnp.minimum(i, j))),
            ],
            out_specs=pl.BlockSpec((TR, TC), lambda i, j, pq: (i, j)),
        ),
        out_shape=jax.ShapeDtypeStruct((ROWS, HALF), F32),
        compiler_params=params(),
        name="final_update",
    )(pq, l_loc, x, y)


def solution(mesh):
    mat_spec = P(("part", "row"), None, "col")

    def local_step(l_blk):
        l_loc = l_blk.reshape(ROWS, HALF)
        pq = jnp.stack([lax.axis_index("row"), lax.axis_index("col")]).astype(jnp.int32)
        first = l_loc[:, 0:LANES].T
        start = [interleave(lax.all_gather(first[NB * h:NB * h + NB], ("col", "row"))) for h in range(2)]
        panels0 = [start[k // 2][k % 2] for k in range(PANELS)]
        panel = panels0[0]
        prev = []
        v_list, w_list, band_list, vec_list, tri_list = [], [], [], [], []
        for k in range(PANELS):
            vt, vts, band, t_mat = panel_qr(k, panel)
            z_part, v_rows = times_matrix(pq, l_loc, vt, vts)
            z = lax.psum(z_part, ("col", "row"))
            wt, panel = make_w(k, z, vt, vts, t_mat, prev, panels0[k + 1] if k + 1 < PANELS else None)
            prev = prev + [vt, wt]
            v_list.append(vt)
            w_list.append(wt)
            band_list.append(band)
            vec_list.append(v_rows)
            tri_list.append(t_mat)
        x, y = prep(pq, v_list, w_list)
        l_out = final_update(pq, l_loc, x, y)
        return l_out.reshape(l_blk.shape), jnp.stack(band_list), jnp.stack(vec_list).transpose(0, 2, 1), jnp.stack(tri_list)

    return jax.shard_map(local_step, mesh=mesh, in_specs=(mat_spec,), out_specs=(mat_spec, P("part"), P(None, ("part", "row"), None), P("part")), check_vma=False)
```

```python
import functools

import jax
import jax.numpy as jnp
from jax import lax
from jax.experimental import pallas as pl
from jax.experimental.pallas import tpu as pltpu
from jax.sharding import PartitionSpec as P

PANELS = 4
NB = 64
NB3 = 3 * NB
LANES = 128
N = 12288
HALF = N // 2
ROWS = N // 4
F32 = jnp.float32
BF16 = jnp.bfloat16
CH = 2048
NCH = N // CH
TR, TC = 512, 1024
NT = ROWS // TR
VMEM_LIMIT = 62 * 1024 * 1024


def lane_of_block(blk):
    pos = (blk % 2) * HALF + (blk // 2) * NB
    return pos // LANES, pos % LANES


def span(start, size):
    return pl.ds(pl.multiple_of(start, size), size)


def split3(x):
    x1 = x.astype(BF16)
    r = x - x1.astype(F32)
    x2 = r.astype(BF16)
    x3 = (r - x2.astype(F32)).astype(BF16)
    return x1, x2, x3


def dot_nn(a, b):
    return lax.dot_general(a, b, (((1,), (0,)), ((), ())), preferred_element_type=F32)


def dot_nt(a, b):
    return lax.dot_general(a, b, (((1,), (1,)), ((), ())), preferred_element_type=F32)


def hi_nn(a, b):
    return lax.dot_general(a, b, (((1,), (0,)), ((), ())), precision=lax.Precision.HIGHEST, preferred_element_type=F32)


def hi_tn(a, b):
    return lax.dot_general(a, b, (((0,), (0,)), ((), ())), precision=lax.Precision.HIGHEST, preferred_element_type=F32)


def stack3(x):
    return jnp.concatenate(split3(x), axis=0)


def fold9(acc):
    r = acc[0:NB] + (acc[NB:LANES] + acc[LANES:NB3])
    return r[:, 0:NB] + (r[:, NB:LANES] + r[:, LANES:NB3])


def iota2(shape, dim):
    return lax.broadcasted_iota(jnp.int32, shape, dim)


def params(**kw):
    return pltpu.CompilerParams(vmem_limit_bytes=VMEM_LIMIT, **kw)


PIECE = ROWS // 2


def interleave_kernel(a_ref, b_ref, o_ref):
    lo = iota2((NB, LANES), 1) < NB
    for m in range(PIECE // LANES):
        a = a_ref[0, :, m * LANES:(m + 1) * LANES]
        b = b_ref[0, :, m * LANES:(m + 1) * LANES]
        at = 2 * m * LANES
        o_ref[:, at:at + LANES] = jnp.where(lo, a, pltpu.roll(b, NB, 1))
        o_ref[:, at + LANES:at + 2 * LANES] = jnp.where(lo, pltpu.roll(a, NB, 1), b)


def interleave(gathered):
    return pl.pallas_call(
        interleave_kernel,
        grid=(2, 2),
        in_specs=[
            pl.BlockSpec((1, NB, PIECE), lambda c, m: (m * 4 + c, 0, 0)),
            pl.BlockSpec((1, NB, PIECE), lambda c, m: (m * 4 + c + 2, 0, 0)),
        ],
        out_specs=pl.BlockSpec((NB, 2 * PIECE), lambda c, m: (0, c * 2 + m)),
        out_shape=jax.ShapeDtypeStruct((NB, N), F32),
        compiler_params=params(),
        name="interleave",
    )(gathered, gathered)


def qr_kernel(k, p_ref, vts_ref, band_ref, t_ref, vt_ref, xb_ref, rt_ref, inv_ref, tau_ref, gram_ref):
    piv_tile, piv_off = lane_of_block(k + 1)
    diag_tile, diag_off = lane_of_block(k)
    piv = slice(piv_tile * LANES, piv_tile * LANES + LANES)

    def copy_in(c, _):
        at = span(c * CH, CH)
        vt_ref[:, at] = p_ref[:, at]
        return 0

    lax.fori_loop(0, NCH, copy_in, 0)
    lane64 = iota2((NB, LANES), 1)
    row64 = iota2((NB, LANES), 0)
    for cls in range(2):
        sl = slice(cls * HALF, cls * HALF + LANES)
        blk = 2 * (lane64 // NB) + cls
        vt_ref[:, sl] = jnp.where(blk >= k + 1, p_ref[:, sl], 0.0)
    rt_ref[...] = jnp.zeros_like(rt_ref)
    inv_ref[...] = jnp.zeros_like(inv_ref)
    tau_ref[...] = jnp.zeros_like(tau_ref)

    for g0 in range(8):
        r0 = 8 * g0
        groups = 8 - g0
        height = 8 * groups
        lane = iota2((height, LANES), 1)
        row_b = r0 + iota2((height, LANES), 0)
        row1 = r0 + iota2((height, 1), 0)

        def step(jj, _, r0=r0, groups=groups, height=height, lane=lane, row_b=row_b, row1=row1):
            j = r0 + jj
            at_piv = lane == piv_off + j

            def dots(c, accs):
                at = span(c * CH, CH)
                xb = jnp.broadcast_to(vt_ref[pl.ds(j, 1), at], (8, CH))
                xb_ref[:, at] = xb
                out = []
                for g in range(groups):
                    prod = vt_ref[r0 + 8 * g:r0 + 8 * g + 8, at] * xb
                    parts = [prod[:, t * LANES:(t + 1) * LANES] for t in range(CH // LANES)]
                    while len(parts) > 1:
                        parts = [parts[i] + parts[i + 1] for i in range(0, len(parts), 2)]
                    out.append(accs[g] + parts[0])
                return tuple(out)

            accs = lax.fori_loop(0, NCH, dots, tuple(jnp.zeros((8, LANES), F32) for _ in range(groups)))
            d = jnp.sum(jnp.concatenate(accs, axis=0), axis=1, keepdims=True)
            pv = jnp.sum(jnp.where(at_piv, vt_ref[r0:NB, piv], 0.0), axis=1, keepdims=True)
            is_j = row1 == j
            nrm2 = jnp.sum(jnp.where(is_j, d, 0.0), axis=0, keepdims=True)
            alpha = jnp.sum(jnp.where(is_j, pv, 0.0), axis=0, keepdims=True)
            norm = jnp.sqrt(nrm2)
            beta = jnp.where(alpha >= 0.0, -norm, norm)
            tau = (beta - alpha) / beta
            inv = 1.0 / (alpha - beta)
            proj = inv * (d - beta * pv)
            s = jnp.where(row1 > j, tau * proj * inv, 0.0)
            xb_ref[:, piv] = xb_ref[:, piv] - jnp.where(lane[0:8] == piv_off + j, beta, 0.0)
            sb = jnp.broadcast_to(s, (height, LANES))

            def update(c, _):
                at = span(c * CH, CH)
                xb = xb_ref[:, at]
                for g in range(groups):
                    sg = sb[8 * g:8 * g + 8]
                    blk = vt_ref[r0 + 8 * g:r0 + 8 * g + 8, at]
                    vt_ref[r0 + 8 * g:r0 + 8 * g + 8, at] = jnp.concatenate(
                        [blk[:, t * LANES:(t + 1) * LANES] - sg * xb[:, t * LANES:(t + 1) * LANES] for t in range(CH // LANES)], axis=1)
                return 0

            lax.fori_loop(0, NCH, update, 0)
            r_col = jnp.where(is_j, beta, jnp.where(row1 > j, pv - s * (alpha - beta), 0.0))
            rt_ref[r0:NB] = jnp.where(lane == j, r_col, rt_ref[r0:NB])
            vt_ref[r0:NB, piv] = jnp.where(at_piv & (row_b > j), 0.0, vt_ref[r0:NB, piv])
            inv_ref[r0:NB] = jnp.where(row_b == j, inv, inv_ref[r0:NB])
            tau_ref[r0:NB] = jnp.where(row_b == j, tau, tau_ref[r0:NB])
            return 0

        lax.fori_loop(0, 8, step, 0)

    vt_ref[:, piv] = jnp.where(lane64 == piv_off + row64, 0.0, vt_ref[:, piv])
    inv_b = inv_ref[...]
    gram_ref[...] = jnp.zeros_like(gram_ref)

    def finish(c, _):
        at = span(c * CH, CH)
        blk = vt_ref[:, at]
        blk = jnp.concatenate([blk[:, t * LANES:(t + 1) * LANES] * inv_b for t in range(CH // LANES)], axis=1)
        lanes = c * CH + iota2((NB, CH), 1)
        blk = jnp.where(lanes == piv_tile * LANES + piv_off + iota2((NB, CH), 0), 1.0, blk)
        st = stack3(blk)
        vts_ref[:, at] = st
        gram_ref[...] += dot_nt(st, st)
        return 0

    lax.fori_loop(0, NCH, finish, 0)
    gram = fold9(gram_ref[...])
    rr = iota2((NB, NB), 0)
    cc = iota2((NB, NB), 1)
    t_mat = jnp.where(rr == cc, tau_ref[:, 0:NB], 0.0)
    size = 1
    while size < NB:
        pair = (rr // (2 * size) == cc // (2 * size)) & ((rr // size) % 2 == 0) & ((cc // size) % 2 == 1)
        t_mat = t_mat - hi_nn(t_mat, hi_nn(jnp.where(pair, gram, 0.0), t_mat))
        size *= 2
    t_ref[...] = t_mat
    diag = p_ref[:, diag_tile * LANES:diag_tile * LANES + LANES].T[diag_off:diag_off + NB]
    band_ref[0:NB] = jnp.where(rr >= cc, diag, 0.0)
    band_ref[NB:LANES] = rt_ref[...].T[0:NB]


def panel_qr(k, panel):
    return pl.pallas_call(
        functools.partial(qr_kernel, k),
        out_shape=(
            jax.ShapeDtypeStruct((NB3, N), BF16),
            jax.ShapeDtypeStruct((LANES, NB), F32),
            jax.ShapeDtypeStruct((NB, NB), F32),
        ),
        scratch_shapes=[
            pltpu.VMEM((NB, N), F32),
            pltpu.VMEM((8, N), F32),
            pltpu.VMEM((NB, LANES), F32),
            pltpu.VMEM((NB, LANES), F32),
            pltpu.VMEM((NB, LANES), F32),
            pltpu.VMEM((NB3, NB3), F32),
        ],
        compiler_params=params(),
        cost_estimate=cost(200),
        name=f"panel_qr{k}",
    )(panel)


LOWER_TILES = [(i, j) for i in range(NT) for j in range(i + 1)]


def whole(ref_tile):
    return (ref_tile[0:NB].astype(F32) + ref_tile[NB:2 * NB].astype(F32)) + ref_tile[2 * NB:NB3].astype(F32)


def av_kernel(ti_ref, tj_ref, pq_ref, l_ref, vtc_ref, vtp_ref, z_ref, vrt_ref, vr_ref, ls_ref, vtr_ref, acc1_ref, acc2_ref):
    step = pl.program_id(0)
    ti = ti_ref[step]
    tj = tj_ref[step]
    proc_row = pq_ref[0]
    proc_col = pq_ref[1]
    upper = (proc_row >> 1) == 1

    @pl.when(step == 0)
    def _():
        acc1_ref[...] = jnp.zeros_like(acc1_ref)
        acc2_ref[...] = jnp.zeros_like(acc2_ref)

        def pick(i, _):
            tile = whole(vtp_ref[:, span(i * LANES, LANES)]).T
            vr_ref[span(i * NB, NB), :] = jnp.where(upper, tile[NB:LANES], tile[0:NB])
            return 0

        lax.fori_loop(0, HALF // LANES, pick, 0)

        def back(m, _):
            tile = vr_ref[span(m * LANES, LANES), :].T
            vrt_ref[:, span(m * LANES, LANES)] = tile
            vtr_ref[:, span(m * LANES, LANES)] = stack3(tile)
            return 0

        lax.fori_loop(0, ROWS // LANES, back, 0)

    cols = span(tj * TC, TC)
    rows = span(ti * TR, TR)
    vc = vtc_ref[:, cols]
    vr = vtr_ref[:, rows]
    pieces = 4
    size = TR // pieces
    for piece in range(pieces):
        sub = slice(piece * size, (piece + 1) * size)
        parts = split3(l_ref[sub, :])
        for n, part in enumerate(parts):
            ls_ref[n, sub, :] = part
        at = span(ti * TR + piece * size, size)
        acc1_ref[at, :] += dot_nt(parts[0], vc) + (dot_nt(parts[1], vc) + dot_nt(parts[2], vc))
    acc2_ref[:, cols] += dot_nn(vr, ls_ref[0])
    acc2_ref[0:2 * NB, cols] += dot_nn(vr[0:2 * NB], ls_ref[1])
    acc2_ref[0:NB, cols] += dot_nn(vr[0:NB], ls_ref[2])

    @pl.when(ti == tj)
    def _():
        diff = proc_row - proc_col
        row = iota2((NB, LANES), 0)
        lane = iota2((NB, LANES), 1)
        on = ((diff & 1) == 0) & (lane == row + (diff >> 1) * NB)
        for i in range(TR // NB):
            tile = l_ref[i * NB:(i + 1) * NB, i * LANES:(i + 1) * LANES]
            diag = jnp.sum(jnp.where(on, tile, 0.0), axis=1, keepdims=True)
            at = span(ti * TR + i * NB, NB)
            acc1_ref[at, 0:NB] = acc1_ref[at, 0:NB] - diag * vr_ref[at, :]

    @pl.when(step == len(LOWER_TILES) - 1)
    def _():
        def out(i, _):
            at = span(i * LANES, LANES)
            blk = acc1_ref[span(i * NB, NB), :]
            blk = blk[:, 0:NB] + (blk[:, NB:2 * NB] + blk[:, 2 * NB:NB3])
            wide = jnp.concatenate([jnp.where(upper, 0.0, blk), jnp.where(upper, blk, 0.0)], axis=0).T
            own = acc2_ref[0:NB, at] + (acc2_ref[NB:2 * NB, at] + acc2_ref[2 * NB:NB3, at])
            for cls in range(2):
                z_ref[:, span(cls * HALF + i * LANES, LANES)] = (
                    jnp.where(proc_col == cls, own, 0.0) + jnp.where((proc_row & 1) == cls, wide, 0.0))
            return 0

        lax.fori_loop(0, HALF // LANES, out, 0)


def cost(mega):
    return pl.CostEstimate(flops=mega * 1000000, bytes_accessed=mega * 1000, transcendentals=0)


def times_matrix(pq, l_loc, vts):
    tile_i = jnp.array([t[0] for t in LOWER_TILES], jnp.int32)
    tile_j = jnp.array([t[1] for t in LOWER_TILES], jnp.int32)
    return pl.pallas_call(
        av_kernel,
        grid_spec=pltpu.PrefetchScalarGridSpec(
            num_scalar_prefetch=3,
            grid=(len(LOWER_TILES),),
            in_specs=[
                pl.BlockSpec((TR, TC), lambda s, ti, tj, pq: (ti[s], tj[s])),
                pl.BlockSpec((NB3, HALF), lambda s, ti, tj, pq: (0, pq[1])),
                pl.BlockSpec((NB3, HALF), lambda s, ti, tj, pq: (0, pq[0] & 1)),
            ],
            out_specs=[
                pl.BlockSpec((NB, N), lambda s, ti, tj, pq: (0, 0)),
                pl.BlockSpec((NB, ROWS), lambda s, ti, tj, pq: (0, 0)),
            ],
            scratch_shapes=[
                pltpu.VMEM((ROWS, NB), F32),
                pltpu.VMEM((3, TR, TC), BF16),
                pltpu.VMEM((NB3, ROWS), BF16),
                pltpu.VMEM((ROWS, NB3), F32),
                pltpu.VMEM((NB3, HALF), F32),
            ],
        ),
        out_shape=(jax.ShapeDtypeStruct((NB, N), F32), jax.ShapeDtypeStruct((NB, ROWS), F32)),
        compiler_params=params(),
        cost_estimate=cost(400),
        name="times_matrix",
    )(tile_i, tile_j, pq, l_loc, vts, vts)


WCH = 1024
NW = N // WCH


def mm6(lhs, m, b1, b2, b3):
    r1 = dot_nn(lhs, b1)
    r2 = dot_nn(lhs[0:2 * m], b2)
    r3 = dot_nn(lhs[0:m], b3)
    return r1[0:m] + ((r1[m:2 * m] + r2[0:m]) + (r1[2 * m:3 * m] + (r2[m:2 * m] + r3)))


def split_rows(tiles, s):
    return jnp.concatenate([t[s * NB:(s + 1) * NB] for t in tiles], axis=0)


def ahead_kernel(k, *refs):
    last = k == PANELS - 1
    count = 2 * k
    vts_ref, prev, refs = refs[0], refs[1:1 + count], refs[1 + count:]
    if last:
        d_ref, acc_ref, lhs_ref = refs
    else:
        at_piv, a0_ref, d_ref, p_ref, acc_ref, lhs_ref = refs[:count], *refs[count:]
    m = NB if last else 2 * NB
    phase = pl.program_id(0)
    chunk = pl.program_id(1)

    @pl.when((phase == 0) & (chunk == 0))
    def _():
        acc_ref[...] = jnp.zeros_like(acc_ref)

    @pl.when(phase == 0)
    def _():
        vs = vts_ref[...]
        for n in range(count):
            acc_ref[n] += dot_nt(prev[n][...], vs)

    @pl.when((phase == 1) & (chunk == 0))
    def _():
        _, off = lane_of_block(k + 1)
        for j in range(k):
            c_v, c_w = fold9(acc_ref[2 * j]), fold9(acc_ref[2 * j + 1])
            mat = jnp.concatenate([c_w, c_v], axis=0).T
            if not last:
                tile = jnp.concatenate([whole(at_piv[2 * j + 1][...]), whole(at_piv[2 * j][...])], axis=0)
                mat = jnp.concatenate([mat, tile.T[off:off + NB]], axis=0)
            lhs_ref[:, j * LANES:(j + 1) * LANES] = stack3(mat)

    @pl.when(phase == 1)
    def _():
        tiles = [ref[...] for ref in prev]
        res = mm6(lhs_ref[...], m, split_rows(tiles, 0), split_rows(tiles, 1), split_rows(tiles, 2))
        d_ref[...] = res[0:NB]
        if not last:
            p_ref[...] = a0_ref[...] - res[NB:2 * NB]


def ahead(k, vts, prev, a0_next):
    last = k == PANELS - 1
    m = NB if last else 2 * NB
    wide = pl.BlockSpec((NB3, WCH), lambda ph, c: (0, c))
    late = pl.BlockSpec((NB, WCH), lambda ph, c: (0, c * ph))
    tile, _ = lane_of_block(k + 1)
    piv = pl.BlockSpec((NB3, LANES), lambda ph, c: (0, tile))
    args = [vts, *prev] + ([] if last else [*prev, a0_next])
    res = pl.pallas_call(
        functools.partial(ahead_kernel, k),
        grid=(2, NW),
        in_specs=[wide] * (1 + 2 * k) + ([] if last else [piv] * (2 * k) + [late]),
        out_specs=[late] * (1 if last else 2),
        out_shape=[jax.ShapeDtypeStruct((NB, N), F32)] * (1 if last else 2),
        scratch_shapes=[pltpu.VMEM((2 * k, NB3, NB3), F32), pltpu.VMEM((3 * m, LANES * k), BF16)],
        compiler_params=params(),
        cost_estimate=cost(100 * k),
        name=f"ahead{k}",
    )(*args)
    return (res[0], None) if last else res


def w_kernel(k, *refs):
    last = k == PANELS - 1
    z_ref, vts_ref, t_ref = refs[:3]
    refs = refs[3:]
    if k > 0:
        d_ref, refs = refs[0], refs[1:]
    if last:
        wts_ref, zs_ref, acc_ref = refs
    else:
        a0_ref, wts_ref, p_ref, zs_ref, acc_ref = refs
    acc_ref[...] = jnp.zeros_like(acc_ref)

    def sums(c, _):
        at = span(c * WCH, WCH)
        z = z_ref[:, at]
        if k > 0:
            z = z - d_ref[:, at]
        zs = stack3(z)
        zs_ref[:, at] = zs
        acc_ref[...] += dot_nt(vts_ref[:, at], zs)
        return 0

    lax.fori_loop(0, NW, sums, 0)
    t_mat = t_ref[...]
    m_mat = hi_tn(t_mat, hi_nn(fold9(acc_ref[...]), t_mat))
    lhs = stack3(jnp.concatenate([t_mat, -0.5 * m_mat], axis=0).T)

    def write_w(c, _):
        at = span(c * WCH, WCH)
        tiles = [zs_ref[:, at], vts_ref[:, at]]
        w = mm6(lhs, NB, split_rows(tiles, 0), split_rows(tiles, 1), split_rows(tiles, 2))
        cls = c // (NW // 2)
        lane = (c - cls * (NW // 2)) * WCH + iota2((NB, WCH), 1)
        wts_ref[:, at] = stack3(jnp.where(2 * (lane // NB) + cls >= k + 1, w, 0.0))
        return 0

    lax.fori_loop(0, NW, write_w, 0)
    if last:
        return
    tile, off = lane_of_block(k + 1)
    piv = slice(tile * LANES, tile * LANES + LANES)
    both = jnp.concatenate([whole(wts_ref[:, piv]), whole(vts_ref[:, piv])], axis=0)
    lhs_p = stack3(both.T[off:off + NB])

    def write_p(c, _):
        at = span(c * WCH, WCH)
        tiles = [vts_ref[:, at], wts_ref[:, at]]
        p_ref[:, at] = a0_ref[:, at] - mm6(lhs_p, NB, split_rows(tiles, 0), split_rows(tiles, 1), split_rows(tiles, 2))
        return 0

    lax.fori_loop(0, NW, write_p, 0)


def make_w(k, z, vts, t_mat, d, a0_next):
    last = k == PANELS - 1
    args = [z, vts, t_mat] + ([d] if k > 0 else []) + ([] if last else [a0_next])
    outs = [jax.ShapeDtypeStruct((NB3, N), BF16)] + ([] if last else [jax.ShapeDtypeStruct((NB, N), F32)])
    res = pl.pallas_call(
        functools.partial(w_kernel, k),
        out_shape=tuple(outs),
        scratch_shapes=[pltpu.VMEM((NB3, N), BF16), pltpu.VMEM((NB3, NB3), F32)],
        compiler_params=params(),
        cost_estimate=cost(100),
        name=f"make_w{k}",
    )(*args)
    return (res[0], None) if last else res


PCH = 1024


def rows_kernel(pq_ref, a_ref, b_ref, x_ref):
    upper = (pq_ref[0] >> 1) == 1
    two = jnp.concatenate([whole(a_ref[...]), whole(b_ref[...])], axis=0).T
    for i in range(PCH // LANES):
        at = i * LANES
        half = jnp.where(upper, two[at + NB:at + LANES], two[at:at + NB])
        for s, part in enumerate(split3(half)):
            x_ref[s, i * NB:(i + 1) * NB, :] = part


def own_rows(pq, a, b):
    spec = pl.BlockSpec((NB3, PCH), lambda c, pq: (0, (pq[0] & 1) * (HALF // PCH) + c))
    return pl.pallas_call(
        rows_kernel,
        grid_spec=pltpu.PrefetchScalarGridSpec(
            num_scalar_prefetch=1,
            grid=(HALF // PCH,),
            in_specs=[spec] * 2,
            out_specs=pl.BlockSpec((3, PCH // 2, LANES), lambda c, pq: (0, c, 0)),
        ),
        out_shape=jax.ShapeDtypeStruct((3, ROWS, LANES), BF16),
        compiler_params=params(),
        cost_estimate=cost(20),
        name="own_rows",
    )(pq, a, b)


UPPER_TILES = [(i, j) for i in range(NT) for j in range(i + 1, NT)]


def final_order():
    order = []
    zeros = list(UPPER_TILES)
    for tile in LOWER_TILES:
        order.append(tile + tile)
        if zeros:
            order.append(tile + zeros.pop())
    return order


def final_kernel(tab_ref, pq_ref, l_ref, *refs):
    xs, ys, o_ref = refs[:4], refs[4:12], refs[12]
    step = pl.program_id(0)
    ti = tab_ref[2, step]
    tj = tab_ref[3, step]

    @pl.when(tj > ti)
    def _():
        o_ref[...] = jnp.zeros_like(o_ref)

    @pl.when(tj <= ti)
    def _():
        x1, x2, x3 = (jnp.concatenate([x[s] for x in xs], axis=1) for s in range(3))
        width = 256
        for c in range(TC // width):
            cols = slice(c * width, (c + 1) * width)
            tiles = [y[:, cols] for y in ys]
            y1, y2, y3 = (split_rows(tiles, s) for s in range(3))
            upd = dot_nn(x3, y1) + dot_nn(x1, y3) + dot_nn(x2, y2) + dot_nn(x2, y1) + dot_nn(x1, y2) + dot_nn(x1, y1)
            rloc = ti * TR + iota2((TR, width), 0)
            cloc = tj * TC + c * width + iota2((TR, width), 1)
            row = ((rloc // NB) * 4 + pq_ref[0]) * NB + rloc % NB
            col = ((cloc // NB) * 2 + pq_ref[1]) * NB + cloc % NB
            keep = (row >= col) & (col >= PANELS * NB)
            o_ref[:, cols] = jnp.where(keep, l_ref[:, cols] - upd, 0.0)


def final_update(pq, l_loc, xs, ys):
    order = final_order()
    table = jnp.array([[t[n] for t in order] for n in range(4)], jnp.int32)
    return pl.pallas_call(
        final_kernel,
        grid_spec=pltpu.PrefetchScalarGridSpec(
            num_scalar_prefetch=2,
            grid=(len(order),),
            in_specs=[pl.BlockSpec((TR, TC), lambda s, tab, pq: (tab[0, s], tab[1, s]))]
            + [pl.BlockSpec((3, TR, LANES), lambda s, tab, pq: (0, tab[0, s], 0))] * 4
            + [pl.BlockSpec((NB3, TC), lambda s, tab, pq: (0, pq[1] * (HALF // TC) + tab[1, s]))] * 8,
            out_specs=pl.BlockSpec((TR, TC), lambda s, tab, pq: (tab[2, s], tab[3, s])),
        ),
        out_shape=jax.ShapeDtypeStruct((ROWS, HALF), F32),
        compiler_params=params(),
        cost_estimate=cost(2000),
        name="final_update",
    )(table, pq, l_loc, *xs, *ys)


def first_panels(first, my_col):
    everyone = ("col", "row")
    out = []
    for h in range(2):
        own = first[NB * h:NB * h + NB]
        low, high = own[:, 0:PIECE], own[:, PIECE:ROWS]
        left = my_col == 0
        keep = jnp.where(left, low, high)
        got = lax.ppermute(jnp.where(left, high, low), "col", [(0, 1), (1, 0)])
        for mine in (jnp.where(left, keep, got), jnp.where(left, got, keep)):
            out.append(interleave(lax.all_gather(mine, everyone)))
    return out


def solution(mesh):
    mat_spec = P(("part", "row"), None, "col")

    def local_step(l_blk):
        l_loc = l_blk.reshape(ROWS, HALF)
        pq = jnp.stack([lax.axis_index("row"), lax.axis_index("col")]).astype(jnp.int32)
        panels0 = first_panels(l_loc[:, 0:LANES].T, lax.axis_index("col"))
        panel = panels0[0]
        prev = []
        v_list, w_list, band_list, vec_list, tri_list, xs = [], [], [], [], [], []
        for k in range(PANELS):
            vts, band, t_mat = panel_qr(k, panel)
            z_part, v_rows = times_matrix(pq, l_loc, vts)
            z = lax.psum(z_part, ("col", "row"))
            a0_next = panels0[k + 1] if k + 1 < PANELS else None
            d = None
            if k > 0:
                d, a0_next = ahead(k, vts, prev, a0_next)
            wts, panel = make_w(k, z, vts, t_mat, d, a0_next)
            prev = prev + [vts, wts]
            v_list.append(vts)
            w_list.append(wts)
            band_list.append(band)
            vec_list.append(v_rows)
            tri_list.append(t_mat)
        xs = [own_rows(pq, group[2 * n], group[2 * n + 1]) for group in (v_list, w_list) for n in range(2)]
        l_out = final_update(pq, l_loc, xs, w_list + v_list)
        return l_out.reshape(l_blk.shape), jnp.stack(band_list), jnp.stack(vec_list).transpose(0, 2, 1), jnp.stack(tri_list)

    return jax.shard_map(local_step, mesh=mesh, in_specs=(mat_spec,), out_specs=(mat_spec, P("part"), P(None, ("part", "row"), None), P("part")), check_vma=False)
```

```python
import functools

import jax
import jax.numpy as jnp
from jax import lax
from jax.experimental import pallas as pl
from jax.experimental.pallas import tpu as pltpu
from jax.sharding import PartitionSpec as P

PANELS = 4
NB = 64
NB3 = 3 * NB
LANES = 128
N = 12288
HALF = N // 2
ROWS = N // 4
F32 = jnp.float32
BF16 = jnp.bfloat16
CH = 2048
NCH = N // CH
TR, TC = 512, 1024
KW = 256
NT = ROWS // TR
VMEM_LIMIT = 62 * 1024 * 1024


def lane_of_block(blk):
    pos = (blk % 2) * HALF + (blk // 2) * NB
    return pos // LANES, pos % LANES


def span(start, size):
    return pl.ds(pl.multiple_of(start, size), size)


def split3(x):
    x1 = x.astype(BF16)
    r = x - x1.astype(F32)
    x2 = r.astype(BF16)
    x3 = (r - x2.astype(F32)).astype(BF16)
    return x1, x2, x3


def dot_nn(a, b):
    return lax.dot_general(a, b, (((1,), (0,)), ((), ())), preferred_element_type=F32)


def dot_nt(a, b):
    return lax.dot_general(a, b, (((1,), (1,)), ((), ())), preferred_element_type=F32)


def hi_nn(a, b):
    return lax.dot_general(a, b, (((1,), (0,)), ((), ())), precision=lax.Precision.HIGHEST, preferred_element_type=F32)


def hi_tn(a, b):
    return lax.dot_general(a, b, (((0,), (0,)), ((), ())), precision=lax.Precision.HIGHEST, preferred_element_type=F32)


def stack3(x):
    return jnp.concatenate(split3(x), axis=0)


def fold9(acc):
    r = acc[0:NB] + (acc[NB:LANES] + acc[LANES:NB3])
    return r[:, 0:NB] + (r[:, NB:LANES] + r[:, LANES:NB3])


def iota2(shape, dim):
    return lax.broadcasted_iota(jnp.int32, shape, dim)


def params(**kw):
    return pltpu.CompilerParams(vmem_limit_bytes=VMEM_LIMIT, **kw)


PIECE = ROWS // 2


def interleave_kernel(a_ref, b_ref, o_ref):
    lo = iota2((NB, LANES), 1) < NB
    for m in range(PIECE // LANES):
        a = a_ref[0, :, m * LANES:(m + 1) * LANES]
        b = b_ref[0, :, m * LANES:(m + 1) * LANES]
        at = 2 * m * LANES
        o_ref[:, at:at + LANES] = jnp.where(lo, a, pltpu.roll(b, NB, 1))
        o_ref[:, at + LANES:at + 2 * LANES] = jnp.where(lo, pltpu.roll(a, NB, 1), b)


def interleave(gathered):
    return pl.pallas_call(
        interleave_kernel,
        grid=(2, 2),
        in_specs=[
            pl.BlockSpec((1, NB, PIECE), lambda c, m: (m * 4 + c, 0, 0)),
            pl.BlockSpec((1, NB, PIECE), lambda c, m: (m * 4 + c + 2, 0, 0)),
        ],
        out_specs=pl.BlockSpec((NB, 2 * PIECE), lambda c, m: (0, c * 2 + m)),
        out_shape=jax.ShapeDtypeStruct((NB, N), F32),
        compiler_params=params(),
        name="interleave",
    )(gathered, gathered)


def qr_kernel(k, p_ref, vts_ref, band_ref, t_ref, vt_ref, xb_ref, rt_ref, inv_ref, tau_ref, gram_ref):
    piv_tile, piv_off = lane_of_block(k + 1)
    diag_tile, diag_off = lane_of_block(k)
    piv = slice(piv_tile * LANES, piv_tile * LANES + LANES)

    def copy_in(c, _):
        at = span(c * CH, CH)
        vt_ref[:, at] = p_ref[:, at]
        return 0

    lax.fori_loop(0, NCH, copy_in, 0)
    lane64 = iota2((NB, LANES), 1)
    row64 = iota2((NB, LANES), 0)
    for cls in range(2):
        sl = slice(cls * HALF, cls * HALF + LANES)
        blk = 2 * (lane64 // NB) + cls
        vt_ref[:, sl] = jnp.where(blk >= k + 1, p_ref[:, sl], 0.0)
    rt_ref[...] = jnp.zeros_like(rt_ref)
    inv_ref[...] = jnp.zeros_like(inv_ref)
    tau_ref[...] = jnp.zeros_like(tau_ref)

    for g0 in range(8):
        r0 = 8 * g0
        groups = 8 - g0
        height = 8 * groups
        lane = iota2((height, LANES), 1)
        row_b = r0 + iota2((height, LANES), 0)
        row1 = r0 + iota2((height, 1), 0)

        def step(jj, _, r0=r0, groups=groups, height=height, lane=lane, row_b=row_b, row1=row1):
            j = r0 + jj
            at_piv = lane == piv_off + j

            def dots(c, accs):
                at = span(c * CH, CH)
                xb = jnp.broadcast_to(vt_ref[pl.ds(j, 1), at], (8, CH))
                xb_ref[:, at] = xb
                out = []
                for g in range(groups):
                    prod = vt_ref[r0 + 8 * g:r0 + 8 * g + 8, at] * xb
                    parts = [prod[:, t * LANES:(t + 1) * LANES] for t in range(CH // LANES)]
                    while len(parts) > 1:
                        parts = [parts[i] + parts[i + 1] for i in range(0, len(parts), 2)]
                    out.append(accs[g] + parts[0])
                return tuple(out)

            accs = lax.fori_loop(0, NCH, dots, tuple(jnp.zeros((8, LANES), F32) for _ in range(groups)))
            d = jnp.sum(jnp.concatenate(accs, axis=0), axis=1, keepdims=True)
            pv = jnp.sum(jnp.where(at_piv, vt_ref[r0:NB, piv], 0.0), axis=1, keepdims=True)
            is_j = row1 == j
            nrm2 = jnp.sum(jnp.where(is_j, d, 0.0), axis=0, keepdims=True)
            alpha = jnp.sum(jnp.where(is_j, pv, 0.0), axis=0, keepdims=True)
            norm = jnp.sqrt(nrm2)
            beta = jnp.where(alpha >= 0.0, -norm, norm)
            tau = (beta - alpha) / beta
            inv = 1.0 / (alpha - beta)
            proj = inv * (d - beta * pv)
            s = jnp.where(row1 > j, tau * proj * inv, 0.0)
            xb_ref[:, piv] = xb_ref[:, piv] - jnp.where(lane[0:8] == piv_off + j, beta, 0.0)
            sb = jnp.broadcast_to(s, (height, LANES))

            def update(c, _):
                at = span(c * CH, CH)
                xb = xb_ref[:, at]
                for g in range(groups):
                    sg = sb[8 * g:8 * g + 8]
                    blk = vt_ref[r0 + 8 * g:r0 + 8 * g + 8, at]
                    vt_ref[r0 + 8 * g:r0 + 8 * g + 8, at] = jnp.concatenate(
                        [blk[:, t * LANES:(t + 1) * LANES] - sg * xb[:, t * LANES:(t + 1) * LANES] for t in range(CH // LANES)], axis=1)
                return 0

            lax.fori_loop(0, NCH, update, 0)
            r_col = jnp.where(is_j, beta, jnp.where(row1 > j, pv - s * (alpha - beta), 0.0))
            rt_ref[r0:NB] = jnp.where(lane == j, r_col, rt_ref[r0:NB])
            vt_ref[r0:NB, piv] = jnp.where(at_piv & (row_b > j), 0.0, vt_ref[r0:NB, piv])
            inv_ref[r0:NB] = jnp.where(row_b == j, inv, inv_ref[r0:NB])
            tau_ref[r0:NB] = jnp.where(row_b == j, tau, tau_ref[r0:NB])
            return 0

        lax.fori_loop(0, 8, step, 0)

    vt_ref[:, piv] = jnp.where(lane64 == piv_off + row64, 0.0, vt_ref[:, piv])
    inv_b = inv_ref[...]
    gram_ref[...] = jnp.zeros_like(gram_ref)

    def finish(c, _):
        at = span(c * CH, CH)
        blk = vt_ref[:, at]
        blk = jnp.concatenate([blk[:, t * LANES:(t + 1) * LANES] * inv_b for t in range(CH // LANES)], axis=1)
        lanes = c * CH + iota2((NB, CH), 1)
        blk = jnp.where(lanes == piv_tile * LANES + piv_off + iota2((NB, CH), 0), 1.0, blk)
        st = stack3(blk)
        vts_ref[:, at] = st
        gram_ref[...] += dot_nt(st, st)
        return 0

    lax.fori_loop(0, NCH, finish, 0)
    gram = fold9(gram_ref[...])
    rr = iota2((NB, NB), 0)
    cc = iota2((NB, NB), 1)
    t_mat = jnp.where(rr == cc, tau_ref[:, 0:NB], 0.0)
    size = 1
    while size < NB:
        pair = (rr // (2 * size) == cc // (2 * size)) & ((rr // size) % 2 == 0) & ((cc // size) % 2 == 1)
        t_mat = t_mat - hi_nn(t_mat, hi_nn(jnp.where(pair, gram, 0.0), t_mat))
        size *= 2
    t_ref[...] = t_mat
    diag = p_ref[:, diag_tile * LANES:diag_tile * LANES + LANES].T[diag_off:diag_off + NB]
    band_ref[0:NB] = jnp.where(rr >= cc, diag, 0.0)
    band_ref[NB:LANES] = rt_ref[...].T[0:NB]


def panel_qr(k, panel):
    return pl.pallas_call(
        functools.partial(qr_kernel, k),
        out_shape=(
            jax.ShapeDtypeStruct((NB3, N), BF16),
            jax.ShapeDtypeStruct((LANES, NB), F32),
            jax.ShapeDtypeStruct((NB, NB), F32),
        ),
        scratch_shapes=[
            pltpu.VMEM((NB, N), F32),
            pltpu.VMEM((8, N), F32),
            pltpu.VMEM((NB, LANES), F32),
            pltpu.VMEM((NB, LANES), F32),
            pltpu.VMEM((NB, LANES), F32),
            pltpu.VMEM((NB3, NB3), F32),
        ],
        compiler_params=params(),
        cost_estimate=cost(200),
        name=f"panel_qr{k}",
    )(panel)


LOWER_TILES = [(i, j) for i in range(NT) for j in range(i + 1)]


def whole(ref_tile):
    return (ref_tile[0:NB].astype(F32) + ref_tile[NB:2 * NB].astype(F32)) + ref_tile[2 * NB:NB3].astype(F32)


def av_kernel(ti_ref, tj_ref, pq_ref, l_ref, vtc_ref, vtp_ref, z_ref, vrt_ref, vr_ref, vtr_ref, acc1_ref, acc2_ref):
    step = pl.program_id(0)
    ti = ti_ref[step]
    tj = tj_ref[step]
    proc_row = pq_ref[0]
    proc_col = pq_ref[1]
    upper = (proc_row >> 1) == 1

    @pl.when(step == 0)
    def _():
        acc1_ref[...] = jnp.zeros_like(acc1_ref)
        acc2_ref[...] = jnp.zeros_like(acc2_ref)

        def pick(i, _):
            tile = whole(vtp_ref[:, span(i * LANES, LANES)]).T
            vr_ref[span(i * NB, NB), :] = jnp.where(upper, tile[NB:LANES], tile[0:NB])
            return 0

        lax.fori_loop(0, HALF // LANES, pick, 0)

        def back(m, _):
            tile = vr_ref[span(m * LANES, LANES), :].T
            vrt_ref[:, span(m * LANES, LANES)] = tile
            vtr_ref[:, span(m * LANES, LANES)] = stack3(tile)
            return 0

        lax.fori_loop(0, ROWS // LANES, back, 0)

    rows = span(ti * TR, TR)
    vr = vtr_ref[:, rows]
    for piece in range(TC // KW):
        sub = slice(piece * KW, (piece + 1) * KW)
        at = span(tj * TC + piece * KW, KW)
        p1, p2, p3 = split3(l_ref[:, sub])
        vc = vtc_ref[:, at]
        acc1_ref[rows, :] += dot_nt(p1, vc) + (dot_nt(p2, vc) + dot_nt(p3, vc))
        r1 = dot_nn(vr, p1)
        r2 = dot_nn(vr[0:2 * NB], p2)
        r3 = dot_nn(vr[0:NB], p3)
        acc2_ref[0:NB, at] += (r1[0:NB] + r2[0:NB]) + r3
        acc2_ref[NB:2 * NB, at] += r1[NB:2 * NB] + r2[NB:2 * NB]
        acc2_ref[2 * NB:NB3, at] += r1[2 * NB:NB3]

    @pl.when(ti == tj)
    def _():
        diff = proc_row - proc_col
        row = iota2((NB, LANES), 0)
        lane = iota2((NB, LANES), 1)
        on = ((diff & 1) == 0) & (lane == row + (diff >> 1) * NB)
        for i in range(TR // NB):
            tile = l_ref[i * NB:(i + 1) * NB, i * LANES:(i + 1) * LANES]
            diag = jnp.sum(jnp.where(on, tile, 0.0), axis=1, keepdims=True)
            at = span(ti * TR + i * NB, NB)
            acc1_ref[at, 0:NB] = acc1_ref[at, 0:NB] - diag * vr_ref[at, :]

    @pl.when(step == len(LOWER_TILES) - 1)
    def _():
        def out(i, _):
            at = span(i * LANES, LANES)
            blk = acc1_ref[span(i * NB, NB), :]
            blk = blk[:, 0:NB] + (blk[:, NB:2 * NB] + blk[:, 2 * NB:NB3])
            wide = jnp.concatenate([jnp.where(upper, 0.0, blk), jnp.where(upper, blk, 0.0)], axis=0).T
            own = acc2_ref[0:NB, at] + (acc2_ref[NB:2 * NB, at] + acc2_ref[2 * NB:NB3, at])
            for cls in range(2):
                z_ref[:, span(cls * HALF + i * LANES, LANES)] = (
                    jnp.where(proc_col == cls, own, 0.0) + jnp.where((proc_row & 1) == cls, wide, 0.0))
            return 0

        lax.fori_loop(0, HALF // LANES, out, 0)


def cost(mega):
    return pl.CostEstimate(flops=mega * 1000000, bytes_accessed=mega * 1000, transcendentals=0)


def times_matrix(pq, l_loc, vts):
    tile_i = jnp.array([t[0] for t in LOWER_TILES], jnp.int32)
    tile_j = jnp.array([t[1] for t in LOWER_TILES], jnp.int32)
    return pl.pallas_call(
        av_kernel,
        grid_spec=pltpu.PrefetchScalarGridSpec(
            num_scalar_prefetch=3,
            grid=(len(LOWER_TILES),),
            in_specs=[
                pl.BlockSpec((TR, TC), lambda s, ti, tj, pq: (ti[s], tj[s])),
                pl.BlockSpec((NB3, HALF), lambda s, ti, tj, pq: (0, pq[1])),
                pl.BlockSpec((NB3, HALF), lambda s, ti, tj, pq: (0, pq[0] & 1)),
            ],
            out_specs=[
                pl.BlockSpec((NB, N), lambda s, ti, tj, pq: (0, 0)),
                pl.BlockSpec((NB, ROWS), lambda s, ti, tj, pq: (0, 0)),
            ],
            scratch_shapes=[
                pltpu.VMEM((ROWS, NB), F32),
                pltpu.VMEM((NB3, ROWS), BF16),
                pltpu.VMEM((ROWS, NB3), F32),
                pltpu.VMEM((NB3, HALF), F32),
            ],
        ),
        out_shape=(jax.ShapeDtypeStruct((NB, N), F32), jax.ShapeDtypeStruct((NB, ROWS), F32)),
        compiler_params=params(),
        cost_estimate=cost(400),
        name="times_matrix",
    )(tile_i, tile_j, pq, l_loc, vts, vts)


WCH = 1024
NW = N // WCH


def mm6(lhs, m, b1, b2, b3):
    r1 = dot_nn(lhs, b1)
    r2 = dot_nn(lhs[0:2 * m], b2)
    r3 = dot_nn(lhs[0:m], b3)
    return r1[0:m] + ((r1[m:2 * m] + r2[0:m]) + (r1[2 * m:3 * m] + (r2[m:2 * m] + r3)))


def split_rows(tiles, s):
    return jnp.concatenate([t[s * NB:(s + 1) * NB] for t in tiles], axis=0)


def ahead_kernel(k, *refs):
    last = k == PANELS - 1
    count = 2 * k
    vts_ref, prev, refs = refs[0], refs[1:1 + count], refs[1 + count:]
    if last:
        d_ref, acc_ref, lhs_ref = refs
    else:
        at_piv, a0_ref, d_ref, p_ref, acc_ref, lhs_ref = refs[:count], *refs[count:]
    m = NB if last else 2 * NB
    phase = pl.program_id(0)
    chunk = pl.program_id(1)

    @pl.when((phase == 0) & (chunk == 0))
    def _():
        acc_ref[...] = jnp.zeros_like(acc_ref)

    @pl.when(phase == 0)
    def _():
        vs = vts_ref[...]
        for n in range(count):
            acc_ref[n] += dot_nt(prev[n][...], vs)

    @pl.when((phase == 1) & (chunk == 0))
    def _():
        _, off = lane_of_block(k + 1)
        for j in range(k):
            c_v, c_w = fold9(acc_ref[2 * j]), fold9(acc_ref[2 * j + 1])
            mat = jnp.concatenate([c_w, c_v], axis=0).T
            if not last:
                tile = jnp.concatenate([whole(at_piv[2 * j + 1][...]), whole(at_piv[2 * j][...])], axis=0)
                mat = jnp.concatenate([mat, tile.T[off:off + NB]], axis=0)
            lhs_ref[:, j * LANES:(j + 1) * LANES] = stack3(mat)

    @pl.when(phase == 1)
    def _():
        tiles = [ref[...] for ref in prev]
        res = mm6(lhs_ref[...], m, split_rows(tiles, 0), split_rows(tiles, 1), split_rows(tiles, 2))
        d_ref[...] = res[0:NB]
        if not last:
            p_ref[...] = a0_ref[...] - res[NB:2 * NB]


def ahead(k, vts, prev, a0_next):
    last = k == PANELS - 1
    m = NB if last else 2 * NB
    wide = pl.BlockSpec((NB3, WCH), lambda ph, c: (0, c))
    late = pl.BlockSpec((NB, WCH), lambda ph, c: (0, c * ph))
    tile, _ = lane_of_block(k + 1)
    piv = pl.BlockSpec((NB3, LANES), lambda ph, c: (0, tile))
    args = [vts, *prev] + ([] if last else [*prev, a0_next])
    res = pl.pallas_call(
        functools.partial(ahead_kernel, k),
        grid=(2, NW),
        in_specs=[wide] * (1 + 2 * k) + ([] if last else [piv] * (2 * k) + [late]),
        out_specs=[late] * (1 if last else 2),
        out_shape=[jax.ShapeDtypeStruct((NB, N), F32)] * (1 if last else 2),
        scratch_shapes=[pltpu.VMEM((2 * k, NB3, NB3), F32), pltpu.VMEM((3 * m, LANES * k), BF16)],
        compiler_params=params(),
        cost_estimate=cost(100 * k),
        name=f"ahead{k}",
    )(*args)
    return (res[0], None) if last else res


def w_kernel(k, *refs):
    last = k == PANELS - 1
    z_ref, vts_ref, t_ref = refs[:3]
    refs = refs[3:]
    if k > 0:
        d_ref, refs = refs[0], refs[1:]
    if last:
        wts_ref, zs_ref, acc_ref = refs
    else:
        a0_ref, wts_ref, p_ref, zs_ref, acc_ref = refs
    acc_ref[...] = jnp.zeros_like(acc_ref)

    def sums(c, _):
        at = span(c * WCH, WCH)
        z = z_ref[:, at]
        if k > 0:
            z = z - d_ref[:, at]
        zs = stack3(z)
        zs_ref[:, at] = zs
        acc_ref[...] += dot_nt(vts_ref[:, at], zs)
        return 0

    lax.fori_loop(0, NW, sums, 0)
    t_mat = t_ref[...]
    m_mat = hi_tn(t_mat, hi_nn(fold9(acc_ref[...]), t_mat))
    lhs = stack3(jnp.concatenate([t_mat, -0.5 * m_mat], axis=0).T)

    def write_w(c, _):
        at = span(c * WCH, WCH)
        tiles = [zs_ref[:, at], vts_ref[:, at]]
        w = mm6(lhs, NB, split_rows(tiles, 0), split_rows(tiles, 1), split_rows(tiles, 2))
        cls = c // (NW // 2)
        lane = (c - cls * (NW // 2)) * WCH + iota2((NB, WCH), 1)
        wts_ref[:, at] = stack3(jnp.where(2 * (lane // NB) + cls >= k + 1, w, 0.0))
        return 0

    lax.fori_loop(0, NW, write_w, 0)
    if last:
        return
    tile, off = lane_of_block(k + 1)
    piv = slice(tile * LANES, tile * LANES + LANES)
    both = jnp.concatenate([whole(wts_ref[:, piv]), whole(vts_ref[:, piv])], axis=0)
    lhs_p = stack3(both.T[off:off + NB])

    def write_p(c, _):
        at = span(c * WCH, WCH)
        tiles = [vts_ref[:, at], wts_ref[:, at]]
        p_ref[:, at] = a0_ref[:, at] - mm6(lhs_p, NB, split_rows(tiles, 0), split_rows(tiles, 1), split_rows(tiles, 2))
        return 0

    lax.fori_loop(0, NW, write_p, 0)


def make_w(k, z, vts, t_mat, d, a0_next):
    last = k == PANELS - 1
    args = [z, vts, t_mat] + ([d] if k > 0 else []) + ([] if last else [a0_next])
    outs = [jax.ShapeDtypeStruct((NB3, N), BF16)] + ([] if last else [jax.ShapeDtypeStruct((NB, N), F32)])
    res = pl.pallas_call(
        functools.partial(w_kernel, k),
        out_shape=tuple(outs),
        scratch_shapes=[pltpu.VMEM((NB3, N), BF16), pltpu.VMEM((NB3, NB3), F32)],
        compiler_params=params(),
        cost_estimate=cost(100),
        name=f"make_w{k}",
    )(*args)
    return (res[0], None) if last else res


PCH = 1024


def place_kernel(pq_ref, a_ref, b_ref, ac_ref, bc_ref, *refs):
    x_ref, y_ref = refs[-2:]
    upper = (pq_ref[0] >> 1) == 1
    two = jnp.concatenate([whole(a_ref[...]), whole(b_ref[...])], axis=0).T
    for i in range(PCH // LANES):
        at = i * LANES
        half = jnp.where(upper, two[at + NB:at + LANES], two[at:at + NB])
        for s, part in enumerate(split3(half)):
            x_ref[s, i * NB:(i + 1) * NB, :] = part
    for s in range(3):
        y_ref[s] = split_rows([ac_ref, bc_ref], s)


def place(pq, old, pos, a, b):
    blocks = HALF // PCH
    row_spec = pl.BlockSpec((NB3, PCH), lambda c, pq: (0, (pq[0] & 1) * blocks + c))
    col_spec = pl.BlockSpec((NB3, PCH), lambda c, pq: (0, pq[1] * blocks + c))
    return pl.pallas_call(
        place_kernel,
        grid_spec=pltpu.PrefetchScalarGridSpec(
            num_scalar_prefetch=1,
            grid=(blocks,),
            in_specs=[row_spec] * 2 + [col_spec] * 2 + [pl.BlockSpec(memory_space=pl.ANY)] * len(old),
            out_specs=[
                pl.BlockSpec((3, PCH // 2, LANES), lambda c, pq: (0, c, pos)),
                pl.BlockSpec((3, LANES, PCH), lambda c, pq: (0, (pos + 2) % 4, c)),
            ],
        ),
        out_shape=(jax.ShapeDtypeStruct((3, ROWS, 512), BF16), jax.ShapeDtypeStruct((3, 512, HALF), BF16)),
        input_output_aliases={5: 0, 6: 1} if old else {},
        compiler_params=params(),
        cost_estimate=cost(20),
        name="place",
    )(pq, a, b, a, b, *old)


UPPER_TILES = [(i, j) for i in range(NT) for j in range(i + 1, NT)]


def final_order():
    order = []
    zeros = list(UPPER_TILES)
    for tile in LOWER_TILES:
        order.append(tile + tile)
        if zeros:
            order.append(tile + zeros.pop())
    return order


def final_kernel(tab_ref, pq_ref, l_ref, x_ref, y_ref, o_ref):
    step = pl.program_id(0)
    ti = tab_ref[2, step]
    tj = tab_ref[3, step]

    @pl.when(tj > ti)
    def _():
        o_ref[...] = jnp.zeros_like(o_ref)

    @pl.when(tj <= ti)
    def _():
        x1, x2, x3 = x_ref[0], x_ref[1], x_ref[2]
        width = 256
        for c in range(TC // width):
            cols = slice(c * width, (c + 1) * width)
            y1, y2, y3 = y_ref[0, :, cols], y_ref[1, :, cols], y_ref[2, :, cols]
            upd = dot_nn(x3, y1) + dot_nn(x1, y3) + dot_nn(x2, y2) + dot_nn(x2, y1) + dot_nn(x1, y2) + dot_nn(x1, y1)
            rloc = ti * TR + iota2((TR, width), 0)
            cloc = tj * TC + c * width + iota2((TR, width), 1)
            row = ((rloc // NB) * 4 + pq_ref[0]) * NB + rloc % NB
            col = ((cloc // NB) * 2 + pq_ref[1]) * NB + cloc % NB
            keep = (row >= col) & (col >= PANELS * NB)
            o_ref[:, cols] = jnp.where(keep, l_ref[:, cols] - upd, 0.0)


def final_update(pq, l_loc, x, y):
    order = final_order()
    table = jnp.array([[t[n] for t in order] for n in range(4)], jnp.int32)
    return pl.pallas_call(
        final_kernel,
        grid_spec=pltpu.PrefetchScalarGridSpec(
            num_scalar_prefetch=2,
            grid=(len(order),),
            in_specs=[
                pl.BlockSpec((TR, TC), lambda s, tab, pq: (tab[0, s], tab[1, s])),
                pl.BlockSpec((3, TR, 512), lambda s, tab, pq: (0, tab[0, s], 0)),
                pl.BlockSpec((3, 512, TC), lambda s, tab, pq: (0, 0, tab[1, s])),
            ],
            out_specs=pl.BlockSpec((TR, TC), lambda s, tab, pq: (tab[2, s], tab[3, s])),
        ),
        out_shape=jax.ShapeDtypeStruct((ROWS, HALF), F32),
        compiler_params=params(),
        cost_estimate=cost(2000),
        name="final_update",
    )(table, pq, l_loc, x, y)


def first_kernel(l_ref, o_ref):
    for m in range(PIECE // LANES):
        tile = l_ref[m * LANES:(m + 1) * LANES, :].T
        o_ref[0, :, m * LANES:(m + 1) * LANES] = tile[0:NB]
        o_ref[1, :, m * LANES:(m + 1) * LANES] = tile[NB:LANES]


def first_columns(l_loc):
    return pl.pallas_call(
        first_kernel,
        grid=(2,),
        in_specs=[pl.BlockSpec((PIECE, LANES), lambda m: (m, 0))],
        out_specs=pl.BlockSpec((2, NB, PIECE), lambda m: (0, 0, m)),
        out_shape=jax.ShapeDtypeStruct((2, NB, ROWS), F32),
        compiler_params=params(),
        name="first_columns",
    )(l_loc)


def first_panels(l_loc, my_col):
    everyone = ("col", "row")
    both = first_columns(l_loc)
    left = my_col == 0
    out = []
    for h in range(2):
        own = both[h]
        if out:
            own, out[0] = lax.optimization_barrier((own, out[0]))
        low, high = own[:, 0:PIECE], own[:, PIECE:ROWS]
        keep = jnp.where(left, low, high)
        got = lax.ppermute(jnp.where(left, high, low), "col", [(0, 1), (1, 0)])
        for mine in (jnp.where(left, keep, got), jnp.where(left, got, keep)):
            out.append(interleave(lax.all_gather(mine, everyone)))
    return out


def solution(mesh):
    mat_spec = P(("part", "row"), None, "col")

    def local_step(l_blk):
        l_loc = l_blk.reshape(ROWS, HALF)
        pq = jnp.stack([lax.axis_index("row"), lax.axis_index("col")]).astype(jnp.int32)
        panels0 = first_panels(l_loc, lax.axis_index("col"))
        panel = panels0[0]
        prev = []
        v_list, w_list, band_list, vec_list, tri_list = [], [], [], [], []
        for k in range(PANELS):
            vts, band, t_mat = panel_qr(k, panel)
            z_part, v_rows = times_matrix(pq, l_loc, vts)
            z = lax.psum(z_part, ("col", "row"))
            a0_next = panels0[k + 1] if k + 1 < PANELS else None
            d = None
            if k > 0:
                d, a0_next = ahead(k, vts, prev, a0_next)
            wts, panel = make_w(k, z, vts, t_mat, d, a0_next)
            prev = prev + [vts, wts]
            v_list.append(vts)
            w_list.append(wts)
            band_list.append(band)
            vec_list.append(v_rows)
            tri_list.append(t_mat)
        factors = ()
        for pos, group in enumerate((v_list, v_list, w_list, w_list)):
            n = 2 * (pos % 2)
            factors = place(pq, factors, pos, group[n], group[n + 1])
        l_out = final_update(pq, l_loc, *factors)
        return l_out.reshape(l_blk.shape), jnp.stack(band_list), jnp.stack(vec_list).transpose(0, 2, 1), jnp.stack(tri_list)

    return jax.shard_map(local_step, mesh=mesh, in_specs=(mat_spec,), out_specs=(mat_spec, P("part"), P(None, ("part", "row"), None), P("part")), check_vma=False)
```
